32 devices in a mesh: row: 8 (over z, y), col: 4 (over x, core).
Axes of the slice: x: 2, y: 2, z: 4, core: 2. Of those that a mesh axis runs over, the one named last changes fastest.
Arguments:
- densities: bfloat16 [4608, 3072], P(('row', 'col')), may hold values from -0.796875 to 0.796875
- counts: int32 [512], P(('row', 'col')), may hold values from 3 to 9
- coulomb: float32 [3072], replicated, may hold values from 0.05 to 1
- energies: float32 [4608], P(('row', 'col')), may hold values from 8 to 64
- vectors: bfloat16 [4608, 64], P(('row', 'col')), may hold values from -0.09375 to 0.09375
Outputs:
- kernel: float32 [4608, 4608], P('row', 'col')
- product: float32 [4608, 64], P(('row', 'col'))
The draws below stay inside these ranges and needn't reach their ends.
All inputs are finite; a program needn't handle non-finite values.
Results may differ from the reference program's by a relative error of at most 0.0095.
Values may be sent and summed in bfloat16 or wider, within the bound.
A program may use at most 128 MiB of HBM per device.

```python
import math
import jax
import jax.numpy as jnp
from jax import lax

G = 3072
NV = 64
SLOT = 9
K_DEV = 16
NK = 512
ROWS = 4608
N_ROW = 8
N_COL = 4


def set_ends(values, own_key, low, largest):
    spot = [jax.random.randint(jax.random.fold_in(own_key, axis), (), 0, length) for axis, length in enumerate(values.shape)]
    main_axis = values.shape.index(max(values.shape))
    beside = spot[:main_axis] + [(spot[main_axis] + 1) % values.shape[main_axis]] + spot[main_axis + 1:]
    return values.at[tuple(spot)].set(low).at[tuple(beside)].set(largest)


def levels(rng, shape, split, smallest, high):
    def one(position, shards_of):
        heights = jax.random.uniform(jax.random.fold_in(jax.random.fold_in(rng, 6), position), (shards_of,), jnp.float32, smallest / len(split), high / len(split))
        return jnp.repeat(jnp.exp(heights), shape[position] // shards_of).reshape((-1,) + (1,) * (len(shape) - position - 1))

    gain = one(*split[0])
    for cut in split[1:]:
        gain = gain * one(*cut)
    return gain


def noise(rng, dims, deviation, reach, shards=(), dtype=jnp.bfloat16):
    array = deviation * jax.random.normal(rng, dims, jnp.float32)
    if shards:
        array = array * levels(rng, dims, shards, -0.22, 0.18)
    return jnp.clip(array, -reach, reach).astype(dtype)


def setup_inputs(seed: int = 0) -> dict:
    seeds = jax.random.split(jax.random.key(seed), 6)
    densities = noise(seeds[0], (ROWS, G), 0.134, 0.796875, ((0, 32),))
    counts = set_ends(jax.random.randint(seeds[1], (NK,), 3, 10), jax.random.fold_in(seeds[1], 1), 3, 9).astype(jnp.int32)
    coulomb = jnp.clip(jnp.exp(jax.random.uniform(seeds[2], (G,), jnp.float32, math.log(0.05), math.log(1.0))), 0.05, 1.0)
    energies = jnp.clip(jnp.exp(math.log(64.0) - 2.0794415 * jax.random.uniform(seeds[3], (ROWS,), jnp.float32) ** levels(seeds[3], (ROWS,), ((0, 32),), -0.2, 0.2)), 8.0, 64.0)
    vectors = noise(seeds[4], (ROWS, NV), ROWS ** -0.5, 0.09375, ((0, 32),))
    return {"densities": densities, "counts": counts, "coulomb": coulomb, "energies": energies, "vectors": vectors}


def reference(densities, counts, coulomb, energies, vectors):
    slots_idx = lax.broadcasted_iota(jnp.int32, (NK, SLOT), 1)
    usable = (slots_idx < counts[:, None]).reshape(NK * SLOT)
    masked = jnp.where(usable[:, None], densities.astype(jnp.float32), 0.0)
    weighted = lax.optimization_barrier((masked * coulomb[None, :]).astype(jnp.bfloat16)).astype(jnp.float32)
    ordered = masked.reshape(N_ROW, N_COL, K_DEV * SLOT, G).transpose(1, 0, 2, 3).reshape(NK * SLOT, G)
    kernel = jnp.dot(weighted, ordered.T, precision=lax.Precision.HIGHEST, preferred_element_type=jnp.float32)
    projected = jnp.dot(masked.T, vectors.astype(jnp.float32), precision=lax.Precision.HIGHEST, preferred_element_type=jnp.float32)
    coupled = jnp.dot(weighted, projected, precision=lax.Precision.HIGHEST, preferred_element_type=jnp.float32)
    diagonal = jnp.where(usable, energies, 0.0)
    product = coupled + diagonal[:, None] * vectors.astype(jnp.float32)
    return kernel, product
```

```python
import functools

import jax
import jax.numpy as jnp
from jax import lax
from jax.experimental import pallas as pl
from jax.experimental.pallas import tpu as pltpu
from jax.sharding import PartitionSpec as P

SLOT = 9
MESH = pl.DeviceIdType.MESH
NT = (((1,), (1,)), ((), ()))
TN = (((0,), (0,)), ((), ()))


def exchange_kernel(n_row, n_col, d_ref, v_ref, coulomb_ref, own_ref, part_ref, prod_ref,
                    cols, rows_raw, weighted, vecs, psend, q, qsend, qrecv, qpiece, qland,
                    local_sem, y_send, y_recv, up_send, down_send, z_recv, x_send, x_recv,
                    core_send, core_recv, v_send, v_recv, p_send, p_recv, q_send, q_recv, c_send, c_recv):
    line, chips = n_row // 2, n_col // 2
    r, c = lax.axis_index("row"), lax.axis_index("col")
    z, y = r // 2, lax.rem(r, 2)
    x, core = c // 2, lax.rem(c, 2)
    other_y, other_core = 1 - y, 1 - core
    block = d_ref.shape[1]
    nv = prod_ref.shape[0]

    barrier = pltpu.get_barrier_semaphore()
    for step in range(1, n_row):
        pl.semaphore_signal(barrier, inc=1, device_id=(lax.rem(r + step, n_row), c), device_id_type=MESH)
    for step in range(1, n_col):
        pl.semaphore_signal(barrier, inc=1, device_id=(r, lax.rem(c + step, n_col)), device_id_type=MESH)
    pl.semaphore_wait(barrier, n_row + n_col - 2)

    partner = (z * 2 + other_y, c)
    sibling = (r, x * 2 + other_core)

    def remote(src, dst, send, recv, device):
        return pltpu.make_async_remote_copy(
            src_ref=src, dst_ref=dst, send_sem=send, recv_sem=recv, device_id=device, device_id_type=MESH)

    def y_copy():
        return remote(d_ref.at[other_y], cols.at[z, y], y_send, y_recv, partner)

    def y_arrival():
        return remote(d_ref.at[other_y], cols.at[z, other_y], y_send, y_recv, partner)

    def up(src, zp, s):
        return remote(src, cols.at[zp, s], up_send.at[zp, s], z_recv.at[zp, s], ((z + 1) * 2 + y, c))

    def down(src, zp, s):
        return remote(src, cols.at[zp, s], down_send.at[zp, s], z_recv.at[zp, s], ((z - 1) * 2 + y, c))

    def x_copy(src, s, step):
        return remote(src, rows_raw.at[s, c], x_send.at[s, step], x_recv.at[s, x],
                      (r, lax.rem(x + step, chips) * 2 + core))

    def x_arrival(s, step):
        xs = lax.rem(x + chips - step, chips)
        return remote(d_ref.at[0], rows_raw.at[s, xs * 2 + core], x_send.at[s, step], x_recv.at[s, xs], sibling)

    def core_copy(src, s, xs):
        return remote(src, rows_raw.at[s, xs * 2 + core], core_send.at[s, xs], core_recv.at[s, xs], sibling)

    def core_arrival(s, xs):
        return remote(d_ref.at[0], rows_raw.at[s, xs * 2 + other_core], core_send.at[s, xs], core_recv.at[s, xs],
                      sibling)

    def spread(src, s):
        @pl.when(z < line - 1)
        def _():
            up(src, z, s).start()

        @pl.when(z > 0)
        def _():
            down(src, z, s).start()

        for step in range(1, chips):
            x_copy(src, s, step).start()
        core_copy(src, s, x).start()

    def relay(zp, s):
        @pl.when((zp < z) & (z < line - 1))
        def _():
            up(cols.at[zp, s], zp, s).start()

        @pl.when((zp > z) & (z > 0))
        def _():
            down(cols.at[zp, s], zp, s).start()

    def z_wait(zp, s):
        remote(cols.at[zp, s], cols.at[zp, s], up_send.at[zp, s], z_recv.at[zp, s], sibling).wait_recv()

    y_copy().start()
    spread(d_ref.at[y], y)
    for step in range(1, n_row):
        remote(v_ref, vecs.at[r], v_send.at[step], v_recv.at[r], (lax.rem(r + step, n_row), c)).start()
    locals_ = [
        pltpu.make_async_copy(d_ref.at[y], cols.at[z, y], local_sem.at[0]),
        pltpu.make_async_copy(d_ref.at[y], rows_raw.at[y, c], local_sem.at[1]),
        pltpu.make_async_copy(v_ref, vecs.at[r], local_sem.at[2]),
    ]
    for copy in locals_:
        copy.start()
    q[...] = jnp.zeros_like(q)
    for copy in locals_:
        copy.wait()

    y_arrival().wait_recv()
    spread(cols.at[z, other_y], other_y)
    late = pltpu.make_async_copy(cols.at[z, other_y], rows_raw.at[other_y, c], local_sem.at[3])
    late.start()

    def share(s):
        for step in range(1, chips):
            xs = lax.rem(x + chips - step, chips)
            x_arrival(s, step).wait_recv()
            core_copy(rows_raw.at[s, xs * 2 + core], s, xs).start()

    def weigh(s):
        for xs in range(chips):
            core_arrival(s, xs).wait_recv()
        for cp in range(n_col):
            weighted[s, cp * block:(cp + 1) * block, :] = (
                rows_raw[s, cp].astype(jnp.float32) * coulomb_ref[y]).astype(jnp.bfloat16)

    share(y)
    for zp in (z - 1, z + 1):
        @pl.when((zp >= 0) & (zp < line))
        def _():
            z_wait(zp, y)
            relay(zp, y)
    weigh(y)
    late.wait()
    share(other_y)
    weigh(other_y)
    for step in range(1, n_row):
        rp = lax.rem(r + step, n_row)
        remote(v_ref, vecs.at[rp], v_send.at[step], v_recv.at[rp], partner).wait_recv()

    def p_copy(rp):
        return remote(psend.at[rp], part_ref.at[rp], p_send.at[rp], p_recv.at[rp], partner)

    def tile(t, carry):
        first = t < 2
        u = jnp.where(first, 0, t - 2)
        d = jnp.where(first, 0, u // 4 + 1)
        turn = jnp.where(first, t, lax.rem(u // 2, 2))
        side = 2 * lax.rem(u, 2) - 1
        zp = z + d * side
        s = jnp.where(turn == 0, y, other_y)

        @pl.when((zp >= 0) & (zp < line))
        def _():
            @pl.when((d > 1) | ((d == 1) & (turn == 1)))
            def _():
                z_wait(zp, s)
                relay(zp, s)

            rp = zp * 2 + s
            away = lax.dot_general(cols[zp, s], weighted[other_y], NT,
                                   preferred_element_type=jnp.float32).astype(jnp.bfloat16)
            psend[rp] = away
            packed = vecs[rp].astype(jnp.float32)
            v = jnp.concatenate([packed[:, :nv], packed[:, nv:]], axis=0).astype(jnp.bfloat16)
            home = lax.dot_general(cols[zp, s], weighted[y], NT, preferred_element_type=jnp.float32)
            own_ref[rp] = home
            p_copy(rp).start()
            q[1] += lax.dot_general(v, away, TN, preferred_element_type=jnp.float32)
            q[0] += lax.dot_general(v, home.astype(jnp.bfloat16), TN, preferred_element_type=jnp.float32)
        return carry

    lax.fori_loop(0, 2 + 4 * (line - 1), tile, 0)

    qsend[...] = q[1].astype(jnp.bfloat16)
    q_copy = remote(qsend, qrecv, q_send, q_recv, partner)
    q_copy.start()
    q_copy.wait()
    total = q[0] + qrecv[...].astype(jnp.float32)
    for cp in range(n_col):
        qpiece[cp] = total[:, cp * block:(cp + 1) * block].astype(jnp.bfloat16)

    def c_copy(step):
        to = lax.rem(c + step, n_col)
        return remote(qpiece.at[to], qland.at[c], c_send.at[step], c_recv.at[c], (r, to))

    for step in range(1, n_col):
        c_copy(step).start()
    answer = qpiece[c].astype(jnp.float32)
    for step in range(1, n_col):
        source = lax.rem(c + step, n_col)
        remote(qpiece.at[0], qland.at[source], c_send.at[step], c_recv.at[source], sibling).wait_recv()
        answer += qland[source].astype(jnp.float32)
    prod_ref[...] = answer

    y_copy().wait_send()
    for step in range(1, n_col):
        c_copy(step).wait_send()
    for step in range(1, n_row):
        remote(v_ref, vecs.at[r], v_send.at[step], v_recv.at[r], partner).wait_send()
    for s in range(2):
        for step in range(1, chips):
            x_copy(d_ref.at[0], s, step).wait_send()
        for xs in range(chips):
            core_copy(d_ref.at[0], s, xs).wait_send()
        for zp in range(line):
            @pl.when((zp <= z) & (z < line - 1))
            def _():
                up(d_ref.at[0], zp, s).wait_send()

            @pl.when((zp >= z) & (z > 0))
            def _():
                down(d_ref.at[0], zp, s).wait_send()
    for rp in range(n_row):
        p_copy(rp).wait()


def body(n_row, n_col, densities, counts, coulomb, energies, vectors):
    rows, depth = densities.shape
    nv = vectors.shape[1]
    half = depth // 2
    line, chips = n_row // 2, n_col // 2
    slot_index = lax.broadcasted_iota(jnp.int32, (counts.shape[0], SLOT), 1)
    usable = (slot_index < counts[:, None]).reshape(rows)
    masked = jnp.where(usable[:, None], densities, jnp.zeros_like(densities))
    halves = jnp.stack([masked[:, :half], masked[:, half:]])
    packed = jnp.concatenate([vectors[:rows // 2], vectors[rows // 2:]], axis=1)
    bf16, f32 = jnp.bfloat16, jnp.float32
    vmem = pl.BlockSpec(memory_space=pltpu.VMEM)
    dma = pltpu.SemaphoreType.DMA
    wide = n_col * rows
    own, part, prod = pl.pallas_call(
        functools.partial(exchange_kernel, n_row, n_col),
        out_shape=(
            jax.ShapeDtypeStruct((n_row, rows, wide), f32),
            jax.ShapeDtypeStruct((n_row, rows, wide), bf16),
            jax.ShapeDtypeStruct((nv, rows), f32),
        ),
        in_specs=[vmem] * 3,
        out_specs=(vmem, vmem, vmem),
        scratch_shapes=[
            pltpu.VMEM((line, 2, rows, half), bf16),
            pltpu.VMEM((2, n_col, rows, half), bf16),
            pltpu.VMEM((2, wide, half), bf16),
            pltpu.VMEM((n_row,) + packed.shape, bf16),
            pltpu.VMEM((n_row, rows, wide), bf16),
            pltpu.VMEM((2, nv, wide), f32),
            pltpu.VMEM((nv, wide), bf16),
            pltpu.VMEM((nv, wide), bf16),
            pltpu.VMEM((n_col, nv, rows), bf16),
            pltpu.VMEM((n_col, nv, rows), bf16),
            dma((4,)), dma, dma, dma((line, 2)), dma((line, 2)), dma((line, 2)),
            dma((2, chips)), dma((2, chips)), dma((2, chips)), dma((2, chips)),
            dma((n_row,)), dma((n_row,)), dma((n_row,)), dma((n_row,)), dma, dma,
            dma((n_col,)), dma((n_col,)),
        ],
        compiler_params=pltpu.CompilerParams(
            collective_id=0, has_side_effects=True, vmem_limit_bytes=60 * 2**20),
    )(halves, packed, coulomb.reshape(2, 1, half))
    kernel = (own + part.astype(f32)).reshape(n_row * rows, wide).T
    diagonal = jnp.where(usable, energies, jnp.zeros_like(energies))
    product = prod.T + diagonal[:, None] * vectors.astype(f32)
    return (kernel, product)


def solution(mesh):
    return jax.shard_map(
        functools.partial(body, mesh.shape["row"], mesh.shape["col"]),
        mesh=mesh,
        in_specs=(
            P(("row", "col"), None),
            P(("row", "col")),
            P(),
            P(("row", "col")),
            P(("row", "col"), None),
        ),
        out_specs=(P("row", "col"), P(("row", "col"), None)),
        check_vma=False,
    )
```

```python
import functools

import jax
import jax.numpy as jnp
from jax import lax
from jax.experimental import pallas as pl
from jax.experimental.pallas import tpu as pltpu
from jax.sharding import PartitionSpec as P

SLOT = 9
MESH = pl.DeviceIdType.MESH
NT = (((1,), (1,)), ((), ()))
NN = (((1,), (0,)), ((), ()))


def pack(v):
    lanes = 128
    rest = v.shape[1] % lanes
    height = v.shape[0] * rest // lanes
    tail = jnp.concatenate(
        [v[j * height:(j + 1) * height, lanes:] for j in range(lanes // rest)], axis=1)
    return jnp.concatenate([v[:, :lanes], tail], axis=0)


def unpack(p, nv, rest):
    lanes = 128
    tail = jnp.concatenate(
        [p[nv:, j * rest:(j + 1) * rest] for j in range(lanes // rest)], axis=0)
    return jnp.concatenate([p[:nv], tail], axis=1)


def exchange_kernel(n_row, n_col, raw_ref, counts_ref, energies_ref, vt_ref, coulomb_ref, own_ref, part_ref, prod_ref,
                    d_ref, v_ref, cols, rows_raw, weighted, vecs, psend, q, qsend, qrecv, qpiece, qland,
                    local_sem, y_send, y_recv, up_send, down_send, z_recv, x_send, x_recv,
                    core_send, core_recv, v_send, v_recv, p_send, p_recv, q_send, q_recv, c_send, c_recv):
    line, chips = n_row // 2, n_col // 2
    r, c = lax.axis_index("row"), lax.axis_index("col")
    z, y = r // 2, lax.rem(r, 2)
    x, core = c // 2, lax.rem(c, 2)
    other_y, other_core = 1 - y, 1 - core
    block = d_ref.shape[1]
    half = d_ref.shape[2]
    nv = prod_ref.shape[0]

    barrier = pltpu.get_barrier_semaphore()
    for step in range(1, n_row):
        pl.semaphore_signal(barrier, inc=1, device_id=(lax.rem(r + step, n_row), c), device_id_type=MESH)
    for step in range(1, n_col):
        pl.semaphore_signal(barrier, inc=1, device_id=(r, lax.rem(c + step, n_col)), device_id_type=MESH)

    kpoints = counts_ref.shape[1]
    counts = counts_ref[...].astype(jnp.float32)
    row_index = lax.broadcasted_iota(jnp.int32, (block, kpoints), 0)
    kpoint = lax.broadcasted_iota(jnp.int32, (block, kpoints), 1)
    slot = row_index - SLOT * kpoint
    inside = (slot >= 0) & (slot < SLOT) & (slot.astype(jnp.float32) < counts)
    usable = jnp.sum(jnp.where(inside, 1.0, 0.0), axis=1, keepdims=True)
    for part in range(2):
        piece = raw_ref[:, part * half:(part + 1) * half].astype(jnp.float32)
        d_ref[part] = jnp.where(usable > 0.5, piece, 0.0).astype(jnp.bfloat16)
    vt = vt_ref[...].astype(jnp.float32)
    v_ref[...] = pack(vt).astype(jnp.bfloat16)
    pl.semaphore_wait(barrier, n_row + n_col - 2)

    partner = (z * 2 + other_y, c)
    sibling = (r, x * 2 + other_core)

    def remote(src, dst, send, recv, device):
        return pltpu.make_async_remote_copy(
            src_ref=src, dst_ref=dst, send_sem=send, recv_sem=recv, device_id=device, device_id_type=MESH)

    def y_copy():
        return remote(d_ref.at[other_y], cols.at[z, y], y_send, y_recv, partner)

    def y_arrival():
        return remote(d_ref.at[other_y], cols.at[z, other_y], y_send, y_recv, partner)

    def up(src, zp, s):
        return remote(src, cols.at[zp, s], up_send.at[zp, s], z_recv.at[zp, s], ((z + 1) * 2 + y, c))

    def down(src, zp, s):
        return remote(src, cols.at[zp, s], down_send.at[zp, s], z_recv.at[zp, s], ((z - 1) * 2 + y, c))

    def x_copy(src, s, step):
        return remote(src, rows_raw.at[s, c], x_send.at[s, step], x_recv.at[s, x],
                      (r, lax.rem(x + step, chips) * 2 + core))

    def x_arrival(s, step):
        xs = lax.rem(x + chips - step, chips)
        return remote(d_ref.at[0], rows_raw.at[s, xs * 2 + core], x_send.at[s, step], x_recv.at[s, xs], sibling)

    def core_copy(src, s, xs):
        return remote(src, rows_raw.at[s, xs * 2 + core], core_send.at[s, xs], core_recv.at[s, xs], sibling)

    def core_arrival(s, xs):
        return remote(d_ref.at[0], rows_raw.at[s, xs * 2 + other_core], core_send.at[s, xs], core_recv.at[s, xs],
                      sibling)

    def spread(src, s):
        @pl.when(z < line - 1)
        def _():
            up(src, z, s).start()

        @pl.when(z > 0)
        def _():
            down(src, z, s).start()

        for step in range(1, chips):
            x_copy(src, s, step).start()
        core_copy(src, s, x).start()

    def relay(zp, s):
        @pl.when((zp < z) & (z < line - 1))
        def _():
            up(cols.at[zp, s], zp, s).start()

        @pl.when((zp > z) & (z > 0))
        def _():
            down(cols.at[zp, s], zp, s).start()

    def z_wait(zp, s):
        remote(cols.at[zp, s], cols.at[zp, s], up_send.at[zp, s], z_recv.at[zp, s], sibling).wait_recv()

    y_copy().start()
    spread(d_ref.at[y], y)
    for step in range(1, n_row):
        remote(v_ref, vecs.at[r], v_send.at[step], v_recv.at[r], (lax.rem(r + step, n_row), c)).start()
    locals_ = [
        pltpu.make_async_copy(d_ref.at[y], cols.at[z, y], local_sem.at[0]),
        pltpu.make_async_copy(d_ref.at[y], rows_raw.at[y, c], local_sem.at[1]),
        pltpu.make_async_copy(v_ref, vecs.at[r], local_sem.at[2]),
    ]
    for copy in locals_:
        copy.start()
    q[...] = jnp.zeros_like(q)
    for copy in locals_:
        copy.wait()

    y_arrival().wait_recv()
    spread(cols.at[z, other_y], other_y)
    late = pltpu.make_async_copy(cols.at[z, other_y], rows_raw.at[other_y, c], local_sem.at[3])
    late.start()

    def share(s):
        for step in range(1, chips):
            xs = lax.rem(x + chips - step, chips)
            x_arrival(s, step).wait_recv()
            core_copy(rows_raw.at[s, xs * 2 + core], s, xs).start()

    def weigh(s):
        for xs in range(chips):
            core_arrival(s, xs).wait_recv()
        for cp in range(n_col):
            weighted[s, cp * block:(cp + 1) * block, :] = (
                rows_raw[s, cp].astype(jnp.float32) * coulomb_ref[y]).astype(jnp.bfloat16)

    share(y)
    for zp in (z - 1, z + 1):
        @pl.when((zp >= 0) & (zp < line))
        def _():
            z_wait(zp, y)
            relay(zp, y)
    weigh(y)
    late.wait()
    share(other_y)
    weigh(other_y)
    for step in range(1, n_row):
        rp = lax.rem(r + step, n_row)
        remote(v_ref, vecs.at[rp], v_send.at[step], v_recv.at[rp], partner).wait_recv()

    def p_copy(rp):
        return remote(psend.at[rp], part_ref.at[rp], p_send.at[rp], p_recv.at[rp], partner)

    def tile(t, carry):
        first = t < 2
        u = jnp.where(first, 0, t - 2)
        d = jnp.where(first, 0, u // 4 + 1)
        turn = jnp.where(first, t, lax.rem(u // 2, 2))
        side = 2 * lax.rem(u, 2) - 1
        zp = z + d * side
        s = jnp.where(turn == 0, y, other_y)

        @pl.when((zp >= 0) & (zp < line))
        def _():
            @pl.when((d > 1) | ((d == 1) & (turn == 1)))
            def _():
                z_wait(zp, s)
                relay(zp, s)

            rp = zp * 2 + s
            away = lax.dot_general(cols[zp, s], weighted[other_y], NT,
                                   preferred_element_type=jnp.float32).astype(jnp.bfloat16)
            psend[rp] = away
            v = unpack(vecs[rp].astype(jnp.float32), nv, block % 128).astype(jnp.bfloat16)
            home = lax.dot_general(cols[zp, s], weighted[y], NT, preferred_element_type=jnp.float32)
            own_ref[rp] = home
            p_copy(rp).start()
            q[1] += lax.dot_general(v, away, NN, preferred_element_type=jnp.float32)
            q[0] += lax.dot_general(v, home.astype(jnp.bfloat16), NN, preferred_element_type=jnp.float32)
        return carry

    lax.fori_loop(0, 2 + 4 * (line - 1), tile, 0)

    qsend[...] = q[1].astype(jnp.bfloat16)
    q_copy = remote(qsend, qrecv, q_send, q_recv, partner)
    q_copy.start()
    q_copy.wait()
    total = q[0] + qrecv[...].astype(jnp.float32)
    for cp in range(n_col):
        qpiece[cp] = total[:, cp * block:(cp + 1) * block].astype(jnp.bfloat16)

    def c_copy(step):
        to = lax.rem(c + step, n_col)
        return remote(qpiece.at[to], qland.at[c], c_send.at[step], c_recv.at[c], (r, to))

    for step in range(1, n_col):
        c_copy(step).start()
    answer = qpiece[c].astype(jnp.float32)
    for step in range(1, n_col):
        source = lax.rem(c + step, n_col)
        remote(qpiece.at[0], qland.at[source], c_send.at[step], c_recv.at[source], sibling).wait_recv()
        answer += qland[source].astype(jnp.float32)
    lane_slot = (lax.broadcasted_iota(jnp.int32, (kpoints, block), 1)
                 - SLOT * lax.broadcasted_iota(jnp.int32, (kpoints, block), 0))
    mine = jnp.where((lane_slot >= 0) & (lane_slot < SLOT), 1.0, 0.0)
    limit = lax.dot_general(jnp.broadcast_to(counts, (8, kpoints)), mine, NN, preferred_element_type=jnp.float32)[:1]
    lane_slot = lax.rem(lax.broadcasted_iota(jnp.int32, (1, block), 1), SLOT).astype(jnp.float32)
    diagonal = jnp.where(lane_slot + 0.5 < limit, energies_ref[...], 0.0)
    prod_ref[...] = answer + diagonal * vt_ref[...].astype(jnp.float32)

    y_copy().wait_send()
    for step in range(1, n_col):
        c_copy(step).wait_send()
    for step in range(1, n_row):
        remote(v_ref, vecs.at[r], v_send.at[step], v_recv.at[r], partner).wait_send()
    for s in range(2):
        for step in range(1, chips):
            x_copy(d_ref.at[0], s, step).wait_send()
        for xs in range(chips):
            core_copy(d_ref.at[0], s, xs).wait_send()
        for zp in range(line):
            @pl.when((zp <= z) & (z < line - 1))
            def _():
                up(d_ref.at[0], zp, s).wait_send()

            @pl.when((zp >= z) & (z > 0))
            def _():
                down(d_ref.at[0], zp, s).wait_send()
    for rp in range(n_row):
        p_copy(rp).wait()


def assemble_kernel(own_ref, part_ref, out_ref):
    n_row, rows, chunk = own_ref.shape
    total = own_ref[...] + part_ref[...].astype(jnp.float32)
    out_ref[...] = total.reshape(n_row * rows, chunk).T


def body(n_row, n_col, densities, counts, coulomb, energies, vectors):
    rows, depth = densities.shape
    nv = vectors.shape[1]
    half = depth // 2
    line, chips = n_row // 2, n_col // 2
    bf16, f32 = jnp.bfloat16, jnp.float32
    packed = jax.eval_shape(pack, jax.ShapeDtypeStruct((nv, rows), bf16))
    vmem = pl.BlockSpec(memory_space=pltpu.VMEM)
    dma = pltpu.SemaphoreType.DMA
    wide = n_col * rows
    own, part, prod = pl.pallas_call(
        functools.partial(exchange_kernel, n_row, n_col),
        out_shape=(
            jax.ShapeDtypeStruct((n_row, rows, wide), f32),
            jax.ShapeDtypeStruct((n_row, rows, wide), bf16),
            jax.ShapeDtypeStruct((nv, rows), f32),
        ),
        in_specs=[vmem] * 5,
        out_specs=(vmem, vmem, vmem),
        scratch_shapes=[
            pltpu.VMEM((2, rows, half), bf16),
            pltpu.VMEM(packed.shape, bf16),
            pltpu.VMEM((line, 2, rows, half), bf16),
            pltpu.VMEM((2, n_col, rows, half), bf16),
            pltpu.VMEM((2, wide, half), bf16),
            pltpu.VMEM((n_row,) + packed.shape, bf16),
            pltpu.VMEM((n_row, rows, wide), bf16),
            pltpu.VMEM((2, nv, wide), f32),
            pltpu.VMEM((nv, wide), bf16),
            pltpu.VMEM((nv, wide), bf16),
            pltpu.VMEM((n_col, nv, rows), bf16),
            pltpu.VMEM((n_col, nv, rows), bf16),
            dma((4,)), dma, dma, dma((line, 2)), dma((line, 2)), dma((line, 2)),
            dma((2, chips)), dma((2, chips)), dma((2, chips)), dma((2, chips)),
            dma((n_row,)), dma((n_row,)), dma((n_row,)), dma((n_row,)), dma, dma,
            dma((n_col,)), dma((n_col,)),
        ],
        compiler_params=pltpu.CompilerParams(
            collective_id=0, has_side_effects=True, vmem_limit_bytes=60 * 2**20),
    )(densities, counts[None], energies[None], vectors.T, coulomb.reshape(2, 1, half))
    chunk = 128
    kernel = pl.pallas_call(
        assemble_kernel,
        out_shape=jax.ShapeDtypeStruct((wide, n_row * rows), f32),
        grid=(pl.cdiv(wide, chunk),),
        in_specs=[pl.BlockSpec((n_row, rows, chunk), lambda i: (0, 0, i))] * 2,
        out_specs=pl.BlockSpec((chunk, n_row * rows), lambda i: (i, 0)),
    )(own, part)
    return (kernel, prod.T)


def solution(mesh):
    return jax.shard_map(
        functools.partial(body, mesh.shape["row"], mesh.shape["col"]),
        mesh=mesh,
        in_specs=(
            P(("row", "col"), None),
            P(("row", "col")),
            P(),
            P(("row", "col")),
            P(("row", "col"), None),
        ),
        out_specs=(P("row", "col"), P(("row", "col"), None)),
        check_vma=False,
    )
```

```python
import functools

import jax
import jax.numpy as jnp
from jax import lax
from jax.experimental import pallas as pl
from jax.experimental.pallas import tpu as pltpu
from jax.sharding import PartitionSpec as P

SLOT = 9
MESH = pl.DeviceIdType.MESH
NT = (((1,), (1,)), ((), ()))
NN = (((1,), (0,)), ((), ()))


def pack(v):
    lanes = 128
    rest = v.shape[1] % lanes
    height = v.shape[0] * rest // lanes
    tail = jnp.concatenate(
        [v[j * height:(j + 1) * height, lanes:] for j in range(lanes // rest)], axis=1)
    return jnp.concatenate([v[:, :lanes], tail], axis=0)


def unpack(p, nv, rest):
    lanes = 128
    tail = jnp.concatenate(
        [p[nv:, j * rest:(j + 1) * rest] for j in range(lanes // rest)], axis=0)
    return jnp.concatenate([p[:nv], tail], axis=1)


def exchange_kernel(n_row, n_col, raw_ref, counts_ref, energies_ref, vt_ref, coulomb_ref, own_ref, part_ref, prod_ref,
                    d_ref, v_ref, cols, rows_raw, weighted, vecs, psend, q, qsend, qrecv, qpiece, qland,
                    local_sem, y_send, y_recv, up_send, down_send, z_recv, x_send, x_recv,
                    core_send, core_recv, v_send, v_recv, p_send, p_recv, q_send, q_recv, c_send, c_recv):
    line, chips = n_row // 2, n_col // 2
    r, c = lax.axis_index("row"), lax.axis_index("col")
    z, y = r // 2, lax.rem(r, 2)
    x, core = c // 2, lax.rem(c, 2)
    other_y, other_core = 1 - y, 1 - core
    block = d_ref.shape[1]
    half = d_ref.shape[2]
    nv = prod_ref.shape[0]

    barrier = pltpu.get_barrier_semaphore()
    for step in range(1, n_row):
        pl.semaphore_signal(barrier, inc=1, device_id=(lax.rem(r + step, n_row), c), device_id_type=MESH)
    for step in range(1, n_col):
        pl.semaphore_signal(barrier, inc=1, device_id=(r, lax.rem(c + step, n_col)), device_id_type=MESH)

    kpoints = counts_ref.shape[1]
    counts = counts_ref[...].astype(jnp.float32)
    row_index = lax.broadcasted_iota(jnp.int32, (block, kpoints), 0)
    kpoint = lax.broadcasted_iota(jnp.int32, (block, kpoints), 1)
    slot = row_index - SLOT * kpoint
    inside = (slot >= 0) & (slot < SLOT) & (slot.astype(jnp.float32) < counts)
    usable = jnp.sum(jnp.where(inside, 1.0, 0.0), axis=1, keepdims=True)
    for part in range(2):
        piece = raw_ref[:, part * half:(part + 1) * half].astype(jnp.float32)
        d_ref[part] = jnp.where(usable > 0.5, piece, 0.0).astype(jnp.bfloat16)
    vt = vt_ref[...].astype(jnp.float32)
    v_ref[...] = pack(vt).astype(jnp.bfloat16)
    pl.semaphore_wait(barrier, n_row + n_col - 2)

    partner = (z * 2 + other_y, c)
    sibling = (r, x * 2 + other_core)

    def remote(src, dst, send, recv, device):
        return pltpu.make_async_remote_copy(
            src_ref=src, dst_ref=dst, send_sem=send, recv_sem=recv, device_id=device, device_id_type=MESH)

    def y_copy():
        return remote(d_ref.at[other_y], cols.at[z, y], y_send, y_recv, partner)

    def y_arrival():
        return remote(d_ref.at[other_y], cols.at[z, other_y], y_send, y_recv, partner)

    def up(src, zp, s):
        return remote(src, cols.at[zp, s], up_send.at[zp, s], z_recv.at[zp, s], ((z + 1) * 2 + y, c))

    def down(src, zp, s):
        return remote(src, cols.at[zp, s], down_send.at[zp, s], z_recv.at[zp, s], ((z - 1) * 2 + y, c))

    def x_copy(src, s, step):
        return remote(src, rows_raw.at[s, c], x_send.at[s, step], x_recv.at[s, x],
                      (r, lax.rem(x + step, chips) * 2 + core))

    def x_arrival(s, step):
        xs = lax.rem(x + chips - step, chips)
        return remote(d_ref.at[0], rows_raw.at[s, xs * 2 + core], x_send.at[s, step], x_recv.at[s, xs], sibling)

    def core_copy(src, s, xs):
        return remote(src, rows_raw.at[s, xs * 2 + core], core_send.at[s, xs], core_recv.at[s, xs], sibling)

    def core_arrival(s, xs):
        return remote(d_ref.at[0], rows_raw.at[s, xs * 2 + other_core], core_send.at[s, xs], core_recv.at[s, xs],
                      sibling)

    def spread(src, s):
        @pl.when(z < line - 1)
        def _():
            up(src, z, s).start()

        @pl.when(z > 0)
        def _():
            down(src, z, s).start()

        for step in range(1, chips):
            x_copy(src, s, step).start()
        core_copy(src, s, x).start()

    def relay(zp, s):
        @pl.when((zp < z) & (z < line - 1))
        def _():
            up(cols.at[zp, s], zp, s).start()

        @pl.when((zp > z) & (z > 0))
        def _():
            down(cols.at[zp, s], zp, s).start()

    def z_wait(zp, s):
        remote(cols.at[zp, s], cols.at[zp, s], up_send.at[zp, s], z_recv.at[zp, s], sibling).wait_recv()

    y_copy().start()
    spread(d_ref.at[y], y)
    for step in range(1, n_row):
        remote(v_ref, vecs.at[r], v_send.at[step], v_recv.at[r], (lax.rem(r + step, n_row), c)).start()
    locals_ = [
        pltpu.make_async_copy(d_ref.at[y], cols.at[z, y], local_sem.at[0]),
        pltpu.make_async_copy(d_ref.at[y], rows_raw.at[y, c], local_sem.at[1]),
        pltpu.make_async_copy(v_ref, vecs.at[r], local_sem.at[2]),
    ]
    for copy in locals_:
        copy.start()
    q[...] = jnp.zeros_like(q)
    for copy in locals_:
        copy.wait()

    y_arrival().wait_recv()
    spread(cols.at[z, other_y], other_y)
    late = pltpu.make_async_copy(cols.at[z, other_y], rows_raw.at[other_y, c], local_sem.at[3])
    late.start()

    def share(s):
        for step in range(1, chips):
            xs = lax.rem(x + chips - step, chips)
            x_arrival(s, step).wait_recv()
            core_copy(rows_raw.at[s, xs * 2 + core], s, xs).start()

    def weigh(s):
        for xs in range(chips):
            core_arrival(s, xs).wait_recv()
        for cp in range(n_col):
            weighted[s, cp * block:(cp + 1) * block, :] = (
                rows_raw[s, cp].astype(jnp.float32) * coulomb_ref[y]).astype(jnp.bfloat16)

    def neighbours(s):
        for zp in (z - 1, z + 1):
            @pl.when((zp >= 0) & (zp < line))
            def _():
                z_wait(zp, s)
                relay(zp, s)

    share(y)
    neighbours(y)
    weigh(y)
    late.wait()
    share(other_y)
    neighbours(other_y)
    weigh(other_y)
    for step in range(1, n_row):
        rp = lax.rem(r + step, n_row)
        remote(v_ref, vecs.at[rp], v_send.at[step], v_recv.at[rp], partner).wait_recv()

    def p_copy(rp):
        return remote(psend.at[rp], part_ref.at[rp], p_send.at[rp], p_recv.at[rp], partner)

    def vector(rp):
        return unpack(vecs[rp].astype(jnp.float32), nv, block % 128).astype(jnp.bfloat16)

    def pair(t, carry):
        zp = z + jnp.where(t == 0, 0, 2 * t - 3)

        @pl.when((zp >= 0) & (zp < line))
        def _():
            both = cols[zp].reshape(2 * block, half)
            away = lax.dot_general(both, weighted[other_y], NT,
                                   preferred_element_type=jnp.float32).astype(jnp.bfloat16)
            for s in range(2):
                tile = away[s * block:(s + 1) * block]
                psend[zp * 2 + s] = tile
                q[1] += lax.dot_general(vector(zp * 2 + s), tile, NN, preferred_element_type=jnp.float32)
            for s in range(2):
                p_copy(zp * 2 + s).start()
            home = lax.dot_general(both, weighted[y], NT, preferred_element_type=jnp.float32)
            for s in range(2):
                tile = home[s * block:(s + 1) * block]
                own_ref[zp * 2 + s] = tile
                q[0] += lax.dot_general(vector(zp * 2 + s), tile.astype(jnp.bfloat16), NN,
                                        preferred_element_type=jnp.float32)
        return carry

    lax.fori_loop(0, 3, pair, 0)

    q_copy = remote(qsend, qrecv, q_send, q_recv, partner)
    slots = 4 * (line - 2)
    last = jnp.where(z == 0, slots - 1, jnp.where(z == line - 1, slots - 2, 4 * (jnp.maximum(z, line - 1 - z) - 2) + 2
                     + jnp.where(z < line - 1 - z, 1, 0)))

    def single(t, carry):
        d = t // 4 + 2
        s = jnp.where(lax.rem(t // 2, 2) == 0, y, other_y)
        zp = z + d * (2 * lax.rem(t, 2) - 1)

        @pl.when((zp >= 0) & (zp < line))
        def _():
            z_wait(zp, s)
            relay(zp, s)
            rp = zp * 2 + s
            v = vector(rp)
            away = lax.dot_general(cols[zp, s], weighted[other_y], NT,
                                   preferred_element_type=jnp.float32).astype(jnp.bfloat16)
            psend[rp] = away
            q[1] += lax.dot_general(v, away, NN, preferred_element_type=jnp.float32)

            @pl.when(t == last)
            def _():
                qsend[...] = q[1].astype(jnp.bfloat16)
                q_copy.start()

            p_copy(rp).start()
            home = lax.dot_general(cols[zp, s], weighted[y], NT, preferred_element_type=jnp.float32)
            own_ref[rp] = home
            q[0] += lax.dot_general(v, home.astype(jnp.bfloat16), NN, preferred_element_type=jnp.float32)
        return carry

    lax.fori_loop(0, slots, single, 0)
    q_copy.wait()
    total = q[0] + qrecv[...].astype(jnp.float32)
    for cp in range(n_col):
        qpiece[cp] = total[:, cp * block:(cp + 1) * block].astype(jnp.bfloat16)

    def c_copy(step):
        to = lax.rem(c + step, n_col)
        return remote(qpiece.at[to], qland.at[c], c_send.at[step], c_recv.at[c], (r, to))

    for step in range(1, n_col):
        c_copy(step).start()
    answer = qpiece[c].astype(jnp.float32)
    for step in range(1, n_col):
        source = lax.rem(c + step, n_col)
        remote(qpiece.at[0], qland.at[source], c_send.at[step], c_recv.at[source], sibling).wait_recv()
        answer += qland[source].astype(jnp.float32)
    lane_slot = (lax.broadcasted_iota(jnp.int32, (kpoints, block), 1)
                 - SLOT * lax.broadcasted_iota(jnp.int32, (kpoints, block), 0))
    mine = jnp.where((lane_slot >= 0) & (lane_slot < SLOT), 1.0, 0.0)
    limit = lax.dot_general(jnp.broadcast_to(counts, (8, kpoints)), mine, NN, preferred_element_type=jnp.float32)[:1]
    lane_slot = lax.rem(lax.broadcasted_iota(jnp.int32, (1, block), 1), SLOT).astype(jnp.float32)
    diagonal = jnp.where(lane_slot + 0.5 < limit, energies_ref[...], 0.0)
    prod_ref[...] = answer + diagonal * vt_ref[...].astype(jnp.float32)

    y_copy().wait_send()
    for step in range(1, n_col):
        c_copy(step).wait_send()
    for step in range(1, n_row):
        remote(v_ref, vecs.at[r], v_send.at[step], v_recv.at[r], partner).wait_send()
    for s in range(2):
        for step in range(1, chips):
            x_copy(d_ref.at[0], s, step).wait_send()
        for xs in range(chips):
            core_copy(d_ref.at[0], s, xs).wait_send()
        for zp in range(line):
            @pl.when((zp <= z) & (z < line - 1))
            def _():
                up(d_ref.at[0], zp, s).wait_send()

            @pl.when((zp >= z) & (z > 0))
            def _():
                down(d_ref.at[0], zp, s).wait_send()
    for rp in range(n_row):
        p_copy(rp).wait()


def assemble_kernel(own_ref, part_ref, out_ref):
    n_row, rows, chunk = own_ref.shape
    total = own_ref[...] + part_ref[...].astype(jnp.float32)
    out_ref[...] = total.reshape(n_row * rows, chunk).T


def body(n_row, n_col, densities, counts, coulomb, energies, vectors):
    rows, depth = densities.shape
    nv = vectors.shape[1]
    half = depth // 2
    line, chips = n_row // 2, n_col // 2
    bf16, f32 = jnp.bfloat16, jnp.float32
    packed = jax.eval_shape(pack, jax.ShapeDtypeStruct((nv, rows), bf16))
    vmem = pl.BlockSpec(memory_space=pltpu.VMEM)
    dma = pltpu.SemaphoreType.DMA
    wide = n_col * rows
    own, part, prod = pl.pallas_call(
        functools.partial(exchange_kernel, n_row, n_col),
        out_shape=(
            jax.ShapeDtypeStruct((n_row, rows, wide), f32),
            jax.ShapeDtypeStruct((n_row, rows, wide), bf16),
            jax.ShapeDtypeStruct((nv, rows), f32),
        ),
        in_specs=[vmem] * 5,
        out_specs=(vmem, vmem, vmem),
        scratch_shapes=[
            pltpu.VMEM((2, rows, half), bf16),
            pltpu.VMEM(packed.shape, bf16),
            pltpu.VMEM((line, 2, rows, half), bf16),
            pltpu.VMEM((2, n_col, rows, half), bf16),
            pltpu.VMEM((2, wide, half), bf16),
            pltpu.VMEM((n_row,) + packed.shape, bf16),
            pltpu.VMEM((n_row, rows, wide), bf16),
            pltpu.VMEM((2, nv, wide), f32),
            pltpu.VMEM((nv, wide), bf16),
            pltpu.VMEM((nv, wide), bf16),
            pltpu.VMEM((n_col, nv, rows), bf16),
            pltpu.VMEM((n_col, nv, rows), bf16),
            dma((4,)), dma, dma, dma((line, 2)), dma((line, 2)), dma((line, 2)),
            dma((2, chips)), dma((2, chips)), dma((2, chips)), dma((2, chips)),
            dma((n_row,)), dma((n_row,)), dma((n_row,)), dma((n_row,)), dma, dma,
            dma((n_col,)), dma((n_col,)),
        ],
        compiler_params=pltpu.CompilerParams(
            collective_id=0, has_side_effects=True, vmem_limit_bytes=60 * 2**20),
    )(densities, counts[None], energies[None], vectors.T, coulomb.reshape(2, 1, half))
    chunk = 128
    kernel = pl.pallas_call(
        assemble_kernel,
        out_shape=jax.ShapeDtypeStruct((wide, n_row * rows), f32),
        grid=(pl.cdiv(wide, chunk),),
        in_specs=[pl.BlockSpec((n_row, rows, chunk), lambda i: (0, 0, i))] * 2,
        out_specs=pl.BlockSpec((chunk, n_row * rows), lambda i: (i, 0)),
    )(own, part)
    return (kernel, prod.T)


def solution(mesh):
    return jax.shard_map(
        functools.partial(body, mesh.shape["row"], mesh.shape["col"]),
        mesh=mesh,
        in_specs=(
            P(("row", "col"), None),
            P(("row", "col")),
            P(),
            P(("row", "col")),
            P(("row", "col"), None),
        ),
        out_specs=(P("row", "col"), P(("row", "col"), None)),
        check_vma=False,
    )
```

```python
import functools

import jax
import jax.numpy as jnp
from jax import lax
from jax.experimental import pallas as pl
from jax.experimental.pallas import tpu as pltpu
from jax.sharding import PartitionSpec as P

SLOT = 9
MESH = pl.DeviceIdType.MESH
NT = (((1,), (1,)), ((), ()))
NN = (((1,), (0,)), ((), ()))


def pack(v):
    lanes = 128
    rest = v.shape[1] % lanes
    height = v.shape[0] * rest // lanes
    tail = jnp.concatenate(
        [v[j * height:(j + 1) * height, lanes:] for j in range(lanes // rest)], axis=1)
    return jnp.concatenate([v[:, :lanes], tail], axis=0)


def unpack(p, nv, rest):
    lanes = 128
    tail = jnp.concatenate(
        [p[nv:, j * rest:(j + 1) * rest] for j in range(lanes // rest)], axis=0)
    return jnp.concatenate([p[:nv], tail], axis=1)


def exchange_kernel(n_row, n_col, raw_ref, counts_ref, energies_ref, vt_ref, coulomb_ref, out_ref, prod_ref,
                    own_ref, part_ref, d_ref, v_ref, cols, rows_raw, weighted, vecs, psend, q, qsend, qrecv, qpiece, qland,
                    local_sem, y_send, y_recv, up_send, down_send, z_recv, x_send, x_recv,
                    core_send, core_recv, v_send, v_recv, p_send, p_recv, q_send, q_recv, c_send, c_recv):
    line, chips = n_row // 2, n_col // 2
    r, c = lax.axis_index("row"), lax.axis_index("col")
    z, y = r // 2, lax.rem(r, 2)
    x, core = c // 2, lax.rem(c, 2)
    other_y, other_core = 1 - y, 1 - core
    block = d_ref.shape[1]
    half = d_ref.shape[2]
    nv = prod_ref.shape[0]

    barrier = pltpu.get_barrier_semaphore()
    for step in range(1, n_row):
        pl.semaphore_signal(barrier, inc=1, device_id=(lax.rem(r + step, n_row), c), device_id_type=MESH)
    for step in range(1, n_col):
        pl.semaphore_signal(barrier, inc=1, device_id=(r, lax.rem(c + step, n_col)), device_id_type=MESH)

    kpoints = counts_ref.shape[1]
    counts = counts_ref[...].astype(jnp.float32)
    row_index = lax.broadcasted_iota(jnp.int32, (block, kpoints), 0)
    kpoint = lax.broadcasted_iota(jnp.int32, (block, kpoints), 1)
    slot = row_index - SLOT * kpoint
    inside = (slot >= 0) & (slot < SLOT) & (slot.astype(jnp.float32) < counts)
    usable = jnp.sum(jnp.where(inside, 1.0, 0.0), axis=1, keepdims=True)
    for part in range(2):
        piece = raw_ref[:, part * half:(part + 1) * half].astype(jnp.float32)
        d_ref[part] = jnp.where(usable > 0.5, piece, 0.0).astype(jnp.bfloat16)
    vt = vt_ref[...].astype(jnp.float32)
    v_ref[...] = pack(vt).astype(jnp.bfloat16)
    pl.semaphore_wait(barrier, n_row + n_col - 2)

    partner = (z * 2 + other_y, c)
    sibling = (r, x * 2 + other_core)

    def remote(src, dst, send, recv, device):
        return pltpu.make_async_remote_copy(
            src_ref=src, dst_ref=dst, send_sem=send, recv_sem=recv, device_id=device, device_id_type=MESH)

    def y_copy():
        return remote(d_ref.at[other_y], cols.at[z, y], y_send, y_recv, partner)

    def y_arrival():
        return remote(d_ref.at[other_y], cols.at[z, other_y], y_send, y_recv, partner)

    def up(src, zp, s):
        return remote(src, cols.at[zp, s], up_send.at[zp, s], z_recv.at[zp, s], ((z + 1) * 2 + y, c))

    def down(src, zp, s):
        return remote(src, cols.at[zp, s], down_send.at[zp, s], z_recv.at[zp, s], ((z - 1) * 2 + y, c))

    def x_copy(src, s, step):
        return remote(src, rows_raw.at[s, c], x_send.at[s, step], x_recv.at[s, x],
                      (r, lax.rem(x + step, chips) * 2 + core))

    def x_arrival(s, step):
        xs = lax.rem(x + chips - step, chips)
        return remote(d_ref.at[0], rows_raw.at[s, xs * 2 + core], x_send.at[s, step], x_recv.at[s, xs], sibling)

    def core_copy(src, s, xs):
        return remote(src, rows_raw.at[s, xs * 2 + core], core_send.at[s, xs], core_recv.at[s, xs], sibling)

    def core_arrival(s, xs):
        return remote(d_ref.at[0], rows_raw.at[s, xs * 2 + other_core], core_send.at[s, xs], core_recv.at[s, xs],
                      sibling)

    def spread(src, s):
        @pl.when(z < line - 1)
        def _():
            up(src, z, s).start()

        @pl.when(z > 0)
        def _():
            down(src, z, s).start()

        for step in range(1, chips):
            x_copy(src, s, step).start()
        core_copy(src, s, x).start()

    def relay(zp, s):
        @pl.when((zp < z) & (z < line - 1))
        def _():
            up(cols.at[zp, s], zp, s).start()

        @pl.when((zp > z) & (z > 0))
        def _():
            down(cols.at[zp, s], zp, s).start()

    def z_wait(zp, s):
        remote(cols.at[zp, s], cols.at[zp, s], up_send.at[zp, s], z_recv.at[zp, s], sibling).wait_recv()

    y_copy().start()
    spread(d_ref.at[y], y)
    for step in range(1, n_row):
        remote(v_ref, vecs.at[r], v_send.at[step], v_recv.at[r], (lax.rem(r + step, n_row), c)).start()
    locals_ = [
        pltpu.make_async_copy(d_ref.at[y], cols.at[z, y], local_sem.at[0]),
        pltpu.make_async_copy(d_ref.at[y], rows_raw.at[y, c], local_sem.at[1]),
        pltpu.make_async_copy(v_ref, vecs.at[r], local_sem.at[2]),
    ]
    for copy in locals_:
        copy.start()
    q[...] = jnp.zeros_like(q)
    for copy in locals_:
        copy.wait()

    y_arrival().wait_recv()
    spread(cols.at[z, other_y], other_y)
    late = pltpu.make_async_copy(cols.at[z, other_y], rows_raw.at[other_y, c], local_sem.at[3])
    late.start()

    def share(s):
        for step in range(1, chips):
            xs = lax.rem(x + chips - step, chips)
            x_arrival(s, step).wait_recv()
            core_copy(rows_raw.at[s, xs * 2 + core], s, xs).start()

    def weigh(s):
        for xs in range(chips):
            core_arrival(s, xs).wait_recv()
        for cp in range(n_col):
            weighted[s, cp * block:(cp + 1) * block, :] = (
                rows_raw[s, cp].astype(jnp.float32) * coulomb_ref[y]).astype(jnp.bfloat16)

    def neighbours(s):
        for zp in (z - 1, z + 1):
            @pl.when((zp >= 0) & (zp < line))
            def _():
                z_wait(zp, s)
                relay(zp, s)

    share(y)
    neighbours(y)
    weigh(y)
    late.wait()
    share(other_y)
    neighbours(other_y)
    weigh(other_y)
    for step in range(1, n_row):
        rp = lax.rem(r + step, n_row)
        remote(v_ref, vecs.at[rp], v_send.at[step], v_recv.at[rp], partner).wait_recv()

    def p_copy(rp):
        return remote(psend.at[rp], part_ref.at[rp], p_send.at[rp], p_recv.at[rp], partner)

    def vector(rp):
        return unpack(vecs[rp].astype(jnp.float32), nv, block % 128).astype(jnp.bfloat16)

    def pair(t, carry):
        zp = z + jnp.where(t == 0, 0, 2 * t - 3)

        @pl.when((zp >= 0) & (zp < line))
        def _():
            both = cols[zp].reshape(2 * block, half)
            away = lax.dot_general(both, weighted[other_y], NT,
                                   preferred_element_type=jnp.float32).astype(jnp.bfloat16)
            for s in range(2):
                tile = away[s * block:(s + 1) * block]
                psend[zp * 2 + s] = tile
                q[1] += lax.dot_general(vector(zp * 2 + s), tile, NN, preferred_element_type=jnp.float32)
            for s in range(2):
                p_copy(zp * 2 + s).start()
            home = lax.dot_general(both, weighted[y], NT, preferred_element_type=jnp.float32)
            for s in range(2):
                tile = home[s * block:(s + 1) * block]
                own_ref[zp * 2 + s] = tile
                q[0] += lax.dot_general(vector(zp * 2 + s), tile.astype(jnp.bfloat16), NN,
                                        preferred_element_type=jnp.float32)
        return carry

    lax.fori_loop(0, 3, pair, 0)

    q_copy = remote(qsend, qrecv, q_send, q_recv, partner)
    slots = 4 * (line - 2)
    last = 4 * (jnp.maximum(z, line - 1 - z) - 2) + 2 + jnp.where(z < line - 1 - z, 1, 0)

    def finish(d, k):
        side = 2 * lax.rem(k, 2) - 1
        zp = z + d * side
        s = jnp.where(k < 2, other_y, y)

        @pl.when((zp >= 0) & (zp < line) & ((d > 0) | (side > 0)))
        def _():
            rp = zp * 2 + s
            p_copy(rp).wait_recv()
            tile = (own_ref[rp] + part_ref[rp].astype(jnp.float32)).T
            for block_index in range(n_row):
                @pl.when(rp == block_index)
                def _():
                    out_ref[:, block_index * block:(block_index + 1) * block] = tile

    def finish_all(d):
        def step(k, carry):
            finish(d, k)
            return carry

        lax.fori_loop(0, 4, step, 0)

    def single(t, carry):
        d = t // 4 + 2
        s = jnp.where(lax.rem(t // 2, 2) == 0, y, other_y)
        zp = z + d * (2 * lax.rem(t, 2) - 1)

        @pl.when((zp >= 0) & (zp < line))
        def _():
            z_wait(zp, s)
            relay(zp, s)
            rp = zp * 2 + s
            v = vector(rp)
            away = lax.dot_general(cols[zp, s], weighted[other_y], NT,
                                   preferred_element_type=jnp.float32).astype(jnp.bfloat16)
            psend[rp] = away
            q[1] += lax.dot_general(v, away, NN, preferred_element_type=jnp.float32)

            @pl.when(t == last)
            def _():
                qsend[...] = q[1].astype(jnp.bfloat16)
                q_copy.start()

            p_copy(rp).start()
            home = lax.dot_general(cols[zp, s], weighted[y], NT, preferred_element_type=jnp.float32)
            own_ref[rp] = home
            q[0] += lax.dot_general(v, home.astype(jnp.bfloat16), NN, preferred_element_type=jnp.float32)

        @pl.when(lax.rem(t, 4) == 3)
        def _():
            finish_all(d - 2)
        return carry

    lax.fori_loop(0, slots, single, 0)
    finish_all(line - 2)
    q_copy.wait()
    total = q[0] + qrecv[...].astype(jnp.float32)
    for cp in range(n_col):
        qpiece[cp] = total[:, cp * block:(cp + 1) * block].astype(jnp.bfloat16)

    def c_copy(step):
        to = lax.rem(c + step, n_col)
        return remote(qpiece.at[to], qland.at[c], c_send.at[step], c_recv.at[c], (r, to))

    for step in range(1, n_col):
        c_copy(step).start()
    answer = qpiece[c].astype(jnp.float32)
    for step in range(1, n_col):
        source = lax.rem(c + step, n_col)
        remote(qpiece.at[0], qland.at[source], c_send.at[step], c_recv.at[source], sibling).wait_recv()
        answer += qland[source].astype(jnp.float32)
    lane_slot = (lax.broadcasted_iota(jnp.int32, (kpoints, block), 1)
                 - SLOT * lax.broadcasted_iota(jnp.int32, (kpoints, block), 0))
    mine = jnp.where((lane_slot >= 0) & (lane_slot < SLOT), 1.0, 0.0)
    limit = lax.dot_general(jnp.broadcast_to(counts, (8, kpoints)), mine, NN, preferred_element_type=jnp.float32)[:1]
    lane_slot = lax.rem(lax.broadcasted_iota(jnp.int32, (1, block), 1), SLOT).astype(jnp.float32)
    diagonal = jnp.where(lane_slot + 0.5 < limit, energies_ref[...], 0.0)
    prod_ref[...] = answer + diagonal * vt_ref[...].astype(jnp.float32)

    finish_all(line - 1)
    y_copy().wait_send()
    for step in range(1, n_col):
        c_copy(step).wait_send()
    for step in range(1, n_row):
        remote(v_ref, vecs.at[r], v_send.at[step], v_recv.at[r], partner).wait_send()
    for s in range(2):
        for step in range(1, chips):
            x_copy(d_ref.at[0], s, step).wait_send()
        for xs in range(chips):
            core_copy(d_ref.at[0], s, xs).wait_send()
        for zp in range(line):
            @pl.when((zp <= z) & (z < line - 1))
            def _():
                up(d_ref.at[0], zp, s).wait_send()

            @pl.when((zp >= z) & (z > 0))
            def _():
                down(d_ref.at[0], zp, s).wait_send()
    for rp in range(n_row):
        p_copy(rp).wait_send()


def body(n_row, n_col, densities, counts, coulomb, energies, vectors):
    rows, depth = densities.shape
    nv = vectors.shape[1]
    half = depth // 2
    line, chips = n_row // 2, n_col // 2
    bf16, f32 = jnp.bfloat16, jnp.float32
    packed = jax.eval_shape(pack, jax.ShapeDtypeStruct((nv, rows), bf16))
    vmem = pl.BlockSpec(memory_space=pltpu.VMEM)
    dma = pltpu.SemaphoreType.DMA
    wide = n_col * rows
    kernel, prod = pl.pallas_call(
        functools.partial(exchange_kernel, n_row, n_col),
        out_shape=(
            jax.ShapeDtypeStruct((wide, n_row * rows), f32),
            jax.ShapeDtypeStruct((nv, rows), f32),
        ),
        in_specs=[vmem] * 5,
        out_specs=(vmem, vmem),
        scratch_shapes=[
            pltpu.VMEM((n_row, rows, wide), f32),
            pltpu.VMEM((n_row, rows, wide), bf16),
            pltpu.VMEM((2, rows, half), bf16),
            pltpu.VMEM(packed.shape, bf16),
            pltpu.VMEM((line, 2, rows, half), bf16),
            pltpu.VMEM((2, n_col, rows, half), bf16),
            pltpu.VMEM((2, wide, half), bf16),
            pltpu.VMEM((n_row,) + packed.shape, bf16),
            pltpu.VMEM((n_row, rows, wide), bf16),
            pltpu.VMEM((2, nv, wide), f32),
            pltpu.VMEM((nv, wide), bf16),
            pltpu.VMEM((nv, wide), bf16),
            pltpu.VMEM((n_col, nv, rows), bf16),
            pltpu.VMEM((n_col, nv, rows), bf16),
            dma((4,)), dma, dma, dma((line, 2)), dma((line, 2)), dma((line, 2)),
            dma((2, chips)), dma((2, chips)), dma((2, chips)), dma((2, chips)),
            dma((n_row,)), dma((n_row,)), dma((n_row,)), dma((n_row,)), dma, dma,
            dma((n_col,)), dma((n_col,)),
        ],
        compiler_params=pltpu.CompilerParams(
            collective_id=0, has_side_effects=True, vmem_limit_bytes=60 * 2**20),
    )(densities, counts[None], energies[None], vectors.T, coulomb.reshape(2, 1, half))
    return (kernel, prod.T)


def solution(mesh):
    return jax.shard_map(
        functools.partial(body, mesh.shape["row"], mesh.shape["col"]),
        mesh=mesh,
        in_specs=(
            P(("row", "col"), None),
            P(("row", "col")),
            P(),
            P(("row", "col")),
            P(("row", "col"), None),
        ),
        out_specs=(P("row", "col"), P(("row", "col"), None)),
        check_vma=False,
    )
```

```python
import functools

import jax
import jax.numpy as jnp
from jax import lax
from jax.experimental import pallas as pl
from jax.experimental.pallas import tpu as pltpu
from jax.sharding import PartitionSpec as P

SLOT = 9
MESH = pl.DeviceIdType.MESH
NT = (((1,), (1,)), ((), ()))
NN = (((1,), (0,)), ((), ()))


def pack(v):
    lanes = 128
    rest = v.shape[1] % lanes
    height = v.shape[0] * rest // lanes
    tail = jnp.concatenate(
        [v[j * height:(j + 1) * height, lanes:] for j in range(lanes // rest)], axis=1)
    return jnp.concatenate([v[:, :lanes], tail], axis=0)


def unpack(p, nv, rest):
    lanes = 128
    tail = jnp.concatenate(
        [p[nv:, j * rest:(j + 1) * rest] for j in range(lanes // rest)], axis=0)
    return jnp.concatenate([p[:nv], tail], axis=1)


def exchange_kernel(n_row, n_col, raw_ref, counts_ref, energies_ref, vt_ref, coulomb_ref, out_ref, prod_ref,
                    own_ref, part_ref, d_ref, v_ref, cols, rows_raw, weighted, vecs, psend, q, qsend, qrecv, qpiece, qland,
                    local_sem, y_send, y_recv, up_send, down_send, z_recv, x_send, x_recv,
                    core_send, core_recv, v_send, v_recv, p_send, p_recv, q_send, q_recv, c_send, c_recv):
    line, chips = n_row // 2, n_col // 2
    r, c = lax.axis_index("row"), lax.axis_index("col")
    z, y = r // 2, lax.rem(r, 2)
    x, core = c // 2, lax.rem(c, 2)
    other_y, other_core = 1 - y, 1 - core
    block = d_ref.shape[1]
    half = d_ref.shape[2]
    nv = prod_ref.shape[0]

    barrier = pltpu.get_barrier_semaphore()
    for step in range(1, n_row):
        pl.semaphore_signal(barrier, inc=1, device_id=(lax.rem(r + step, n_row), c), device_id_type=MESH)
    for step in range(1, n_col):
        pl.semaphore_signal(barrier, inc=1, device_id=(r, lax.rem(c + step, n_col)), device_id_type=MESH)

    kpoints = counts_ref.shape[1]
    counts = counts_ref[...].astype(jnp.float32)
    row_index = lax.broadcasted_iota(jnp.int32, (block, kpoints), 0)
    kpoint = lax.broadcasted_iota(jnp.int32, (block, kpoints), 1)
    slot = row_index - SLOT * kpoint
    inside = (slot >= 0) & (slot < SLOT) & (slot.astype(jnp.float32) < counts)
    usable = jnp.sum(jnp.where(inside, 1.0, 0.0), axis=1, keepdims=True)
    for part in range(2):
        piece = raw_ref[:, part * half:(part + 1) * half].astype(jnp.float32)
        d_ref[part] = jnp.where(usable > 0.5, piece, 0.0).astype(jnp.bfloat16)
    vt = vt_ref[...].astype(jnp.float32)
    v_ref[...] = pack(vt).astype(jnp.bfloat16)
    pl.semaphore_wait(barrier, n_row + n_col - 2)

    partner = (z * 2 + other_y, c)
    sibling = (r, x * 2 + other_core)

    def remote(src, dst, send, recv, device):
        return pltpu.make_async_remote_copy(
            src_ref=src, dst_ref=dst, send_sem=send, recv_sem=recv, device_id=device, device_id_type=MESH)

    def y_copy():
        return remote(d_ref.at[other_y], cols.at[z, y], y_send, y_recv, partner)

    def y_arrival():
        return remote(d_ref.at[other_y], cols.at[z, other_y], y_send, y_recv, partner)

    def up(src, zp, s):
        return remote(src, cols.at[zp, s], up_send.at[zp, s], z_recv.at[zp, s], ((z + 1) * 2 + y, c))

    def down(src, zp, s):
        return remote(src, cols.at[zp, s], down_send.at[zp, s], z_recv.at[zp, s], ((z - 1) * 2 + y, c))

    def x_copy(src, s, step):
        return remote(src, rows_raw.at[s, c], x_send.at[s, step], x_recv.at[s, x],
                      (r, lax.rem(x + step, chips) * 2 + core))

    def x_arrival(s, step):
        xs = lax.rem(x + chips - step, chips)
        return remote(d_ref.at[0], rows_raw.at[s, xs * 2 + core], x_send.at[s, step], x_recv.at[s, xs], sibling)

    def core_copy(src, s, xs):
        return remote(src, rows_raw.at[s, xs * 2 + core], core_send.at[s, xs], core_recv.at[s, xs], sibling)

    def core_arrival(s, xs):
        return remote(d_ref.at[0], rows_raw.at[s, xs * 2 + other_core], core_send.at[s, xs], core_recv.at[s, xs],
                      sibling)

    def spread(src, s):
        @pl.when(z < line - 1)
        def _():
            up(src, z, s).start()

        @pl.when(z > 0)
        def _():
            down(src, z, s).start()

        for step in range(1, chips):
            x_copy(src, s, step).start()
        core_copy(src, s, x).start()

    def relay(zp, s):
        @pl.when((zp < z) & (z < line - 1))
        def _():
            up(cols.at[zp, s], zp, s).start()

        @pl.when((zp > z) & (z > 0))
        def _():
            down(cols.at[zp, s], zp, s).start()

    def z_wait(zp, s):
        remote(cols.at[zp, s], cols.at[zp, s], up_send.at[zp, s], z_recv.at[zp, s], sibling).wait_recv()

    y_copy().start()
    spread(d_ref.at[y], y)
    for step in range(1, n_row):
        remote(v_ref, vecs.at[r], v_send.at[step], v_recv.at[r], (lax.rem(r + step, n_row), c)).start()
    locals_ = [
        pltpu.make_async_copy(d_ref.at[y], cols.at[z, y], local_sem.at[0]),
        pltpu.make_async_copy(d_ref.at[y], rows_raw.at[y, c], local_sem.at[1]),
        pltpu.make_async_copy(v_ref, vecs.at[r], local_sem.at[2]),
    ]
    for copy in locals_:
        copy.start()
    q[...] = jnp.zeros_like(q)
    for copy in locals_:
        copy.wait()

    y_arrival().wait_recv()
    spread(cols.at[z, other_y], other_y)
    late = pltpu.make_async_copy(cols.at[z, other_y], rows_raw.at[other_y, c], local_sem.at[3])
    late.start()

    def share(s):
        for step in range(1, chips):
            xs = lax.rem(x + chips - step, chips)
            x_arrival(s, step).wait_recv()
            core_copy(rows_raw.at[s, xs * 2 + core], s, xs).start()

    def weigh(s):
        for xs in range(chips):
            core_arrival(s, xs).wait_recv()
        for cp in range(n_col):
            weighted[s, cp * block:(cp + 1) * block, :] = (
                rows_raw[s, cp].astype(jnp.float32) * coulomb_ref[y]).astype(jnp.bfloat16)

    def neighbours(s):
        for zp in (z - 1, z + 1):
            @pl.when((zp >= 0) & (zp < line))
            def _():
                z_wait(zp, s)
                relay(zp, s)

    share(y)
    neighbours(y)
    weigh(y)
    late.wait()
    share(other_y)
    neighbours(other_y)
    weigh(other_y)
    for step in range(1, n_row):
        rp = lax.rem(r + step, n_row)
        remote(v_ref, vecs.at[rp], v_send.at[step], v_recv.at[rp], partner).wait_recv()

    def p_copy(rp):
        return remote(psend.at[rp], part_ref.at[rp], p_send.at[rp], p_recv.at[rp], partner)

    def vector(rp):
        return unpack(vecs[rp].astype(jnp.float32), nv, block % 128).astype(jnp.bfloat16)

    def pair(t, carry):
        zp = z + jnp.where(t == 0, 0, 2 * t - 3)

        @pl.when((zp >= 0) & (zp < line))
        def _():
            both = cols[zp].reshape(2 * block, half)
            away = lax.dot_general(both, weighted[other_y], NT,
                                   preferred_element_type=jnp.float32).astype(jnp.bfloat16)
            for s in range(2):
                tile = away[s * block:(s + 1) * block]
                psend[zp * 2 + s] = tile
                q[1] += lax.dot_general(vector(zp * 2 + s), tile, NN, preferred_element_type=jnp.float32)
            for s in range(2):
                p_copy(zp * 2 + s).start()
            home = lax.dot_general(both, weighted[y], NT, preferred_element_type=jnp.float32)
            for s in range(2):
                tile = home[s * block:(s + 1) * block]
                own_ref[zp * 2 + s] = tile
                q[0] += lax.dot_general(vector(zp * 2 + s), tile.astype(jnp.bfloat16), NN,
                                        preferred_element_type=jnp.float32)
        return carry

    lax.fori_loop(0, 3, pair, 0)

    q_copy = remote(qsend, qrecv, q_send, q_recv, partner)
    slots = 4 * (line - 2)
    last = 4 * (jnp.maximum(z, line - 1 - z) - 2) + 2 + jnp.where(z < line - 1 - z, 1, 0)

    def finish(d, k):
        side = 2 * lax.rem(k, 2) - 1
        zp = z + d * side
        s = jnp.where(k < 2, other_y, y)

        @pl.when((zp >= 0) & (zp < line) & ((d > 0) | (side > 0)))
        def _():
            rp = zp * 2 + s
            p_copy(rp).wait_recv()
            tile = (own_ref[rp] + part_ref[rp].astype(jnp.float32)).T.astype(jnp.bfloat16)
            for block_index in range(n_row):
                @pl.when(rp == block_index)
                def _():
                    out_ref[:, block_index * block:(block_index + 1) * block] = tile

    def finish_all(d):
        def step(k, carry):
            finish(d, k)
            return carry

        lax.fori_loop(0, 4, step, 0)

    def single(t, carry):
        d = t // 4 + 2
        s = jnp.where(lax.rem(t // 2, 2) == 0, y, other_y)
        zp = z + d * (2 * lax.rem(t, 2) - 1)

        @pl.when((zp >= 0) & (zp < line))
        def _():
            z_wait(zp, s)
            relay(zp, s)
            rp = zp * 2 + s
            v = vector(rp)
            away = lax.dot_general(cols[zp, s], weighted[other_y], NT,
                                   preferred_element_type=jnp.float32).astype(jnp.bfloat16)
            psend[rp] = away
            q[1] += lax.dot_general(v, away, NN, preferred_element_type=jnp.float32)

            @pl.when(t == last)
            def _():
                qsend[...] = q[1].astype(jnp.bfloat16)
                q_copy.start()

            p_copy(rp).start()
            home = lax.dot_general(cols[zp, s], weighted[y], NT, preferred_element_type=jnp.float32)
            own_ref[rp] = home
            q[0] += lax.dot_general(v, home.astype(jnp.bfloat16), NN, preferred_element_type=jnp.float32)

        @pl.when(lax.rem(t, 4) == 1)
        def _():
            finish_all(d - 2)

        @pl.when(t == slots - 3)
        def _():
            finish_all(line - 2)
        return carry

    lax.fori_loop(0, slots, single, 0)
    q_copy.wait()
    total = q[0] + qrecv[...].astype(jnp.float32)
    for cp in range(n_col):
        qpiece[cp] = total[:, cp * block:(cp + 1) * block].astype(jnp.bfloat16)

    def c_copy(step):
        to = lax.rem(c + step, n_col)
        return remote(qpiece.at[to], qland.at[c], c_send.at[step], c_recv.at[c], (r, to))

    for step in range(1, n_col):
        c_copy(step).start()
    answer = qpiece[c].astype(jnp.float32)
    for step in range(1, n_col):
        source = lax.rem(c + step, n_col)
        remote(qpiece.at[0], qland.at[source], c_send.at[step], c_recv.at[source], sibling).wait_recv()
        answer += qland[source].astype(jnp.float32)
    lane_slot = (lax.broadcasted_iota(jnp.int32, (kpoints, block), 1)
                 - SLOT * lax.broadcasted_iota(jnp.int32, (kpoints, block), 0))
    mine = jnp.where((lane_slot >= 0) & (lane_slot < SLOT), 1.0, 0.0)
    limit = lax.dot_general(jnp.broadcast_to(counts, (8, kpoints)), mine, NN, preferred_element_type=jnp.float32)[:1]
    lane_slot = lax.rem(lax.broadcasted_iota(jnp.int32, (1, block), 1), SLOT).astype(jnp.float32)
    diagonal = jnp.where(lane_slot + 0.5 < limit, energies_ref[...], 0.0)
    prod_ref[...] = answer + diagonal * vt_ref[...].astype(jnp.float32)

    finish_all(line - 1)
    y_copy().wait_send()
    for step in range(1, n_col):
        c_copy(step).wait_send()
    for step in range(1, n_row):
        remote(v_ref, vecs.at[r], v_send.at[step], v_recv.at[r], partner).wait_send()
    for s in range(2):
        for step in range(1, chips):
            x_copy(d_ref.at[0], s, step).wait_send()
        for xs in range(chips):
            core_copy(d_ref.at[0], s, xs).wait_send()
        for zp in range(line):
            @pl.when((zp <= z) & (z < line - 1))
            def _():
                up(d_ref.at[0], zp, s).wait_send()

            @pl.when((zp >= z) & (z > 0))
            def _():
                down(d_ref.at[0], zp, s).wait_send()
    for rp in range(n_row):
        p_copy(rp).wait_send()


def body(n_row, n_col, densities, counts, coulomb, energies, vectors):
    rows, depth = densities.shape
    nv = vectors.shape[1]
    half = depth // 2
    line, chips = n_row // 2, n_col // 2
    bf16, f32 = jnp.bfloat16, jnp.float32
    packed = jax.eval_shape(pack, jax.ShapeDtypeStruct((nv, rows), bf16))
    vmem = pl.BlockSpec(memory_space=pltpu.VMEM)
    dma = pltpu.SemaphoreType.DMA
    wide = n_col * rows
    kernel, prod = pl.pallas_call(
        functools.partial(exchange_kernel, n_row, n_col),
        out_shape=(
            jax.ShapeDtypeStruct((wide, n_row * rows), bf16),
            jax.ShapeDtypeStruct((nv, rows), f32),
        ),
        in_specs=[vmem] * 5,
        out_specs=(vmem, vmem),
        scratch_shapes=[
            pltpu.VMEM((n_row, rows, wide), f32),
            pltpu.VMEM((n_row, rows, wide), bf16),
            pltpu.VMEM((2, rows, half), bf16),
            pltpu.VMEM(packed.shape, bf16),
            pltpu.VMEM((line, 2, rows, half), bf16),
            pltpu.VMEM((2, n_col, rows, half), bf16),
            pltpu.VMEM((2, wide, half), bf16),
            pltpu.VMEM((n_row,) + packed.shape, bf16),
            pltpu.VMEM((n_row, rows, wide), bf16),
            pltpu.VMEM((2, nv, wide), f32),
            pltpu.VMEM((nv, wide), bf16),
            pltpu.VMEM((nv, wide), bf16),
            pltpu.VMEM((n_col, nv, rows), bf16),
            pltpu.VMEM((n_col, nv, rows), bf16),
            dma((4,)), dma, dma, dma((line, 2)), dma((line, 2)), dma((line, 2)),
            dma((2, chips)), dma((2, chips)), dma((2, chips)), dma((2, chips)),
            dma((n_row,)), dma((n_row,)), dma((n_row,)), dma((n_row,)), dma, dma,
            dma((n_col,)), dma((n_col,)),
        ],
        compiler_params=pltpu.CompilerParams(
            collective_id=0, has_side_effects=True, vmem_limit_bytes=60 * 2**20),
    )(densities, counts[None], energies[None], vectors.T, coulomb.reshape(2, 1, half))
    return (kernel.astype(f32), prod.T)


def solution(mesh):
    return jax.shard_map(
        functools.partial(body, mesh.shape["row"], mesh.shape["col"]),
        mesh=mesh,
        in_specs=(
            P(("row", "col"), None),
            P(("row", "col")),
            P(),
            P(("row", "col")),
            P(("row", "col"), None),
        ),
        out_specs=(P("row", "col"), P(("row", "col"), None)),
        check_vma=False,
    )
```
